32 devices in a mesh: ep: 16 (over z, y, x), tp: 2 (over core).
Axes of the slice: x: 2, y: 2, z: 4, core: 2. Of those that a mesh axis runs over, the one named last changes fastest.
Arguments:
- tokens: bfloat16 [256, 7168], P('ep', 'tp'), may hold values from -6 to 6
- route_ids: int32 [256, 8], P('ep'), may hold values from 0 to 15, all different within a row; in each aligned block of 16 rows (0 to 15, 16 to 31, ...) at most 16 rows name the same one
- expert_slot: int32 [16], replicated, may hold values from 0 to 15, each once
- router_weight: bfloat16 [7168, 16], P('tp'), may hold values from -0.0625 to 0.0625
- expert_gate: bfloat16 [16, 7168, 1024], P('ep', 'tp'), may hold values from -0.0625 to 0.0625
- expert_up: bfloat16 [16, 7168, 1024], P('ep', 'tp'), may hold values from -0.0625 to 0.0625
- expert_down: bfloat16 [16, 1024, 7168], P('ep', None, 'tp'), may hold values from -0.1875 to 0.1875
- shared_gate: bfloat16 [7168, 1024], P('tp', 'ep'), may hold values from -0.0625 to 0.0625
- shared_up: bfloat16 [7168, 1024], P('tp', 'ep'), may hold values from -0.0625 to 0.0625
- shared_down: bfloat16 [1024, 7168], P('ep', 'tp'), may hold values from -0.1875 to 0.1875
Outputs:
- mixed: bfloat16 [256, 7168], P('ep', 'tp')
The draws below stay inside these ranges and needn't reach their ends.
Inputs may be any that keep to these rules, and one draw needn't show every extreme that they name: `route_ids`: each row names 8 different experts. Among the rows of one device (the aligned blocks of 16 rows) no expert is named more than 16 times, and in some blocks one expert is named exactly 16 times. A permutation of 0 to 15; the weights of expert e lie in row expert_slot[e] of the expert weight arrays.
All inputs are finite; a program needn't handle non-finite values.
Results may differ from the reference program's by a relative error of at most 0.003.
Values may be sent and summed in bfloat16 or wider, within the bound.
A program may use at most 128 MiB of HBM per device.

```python
import math
import jax
import jax.numpy as jnp
import numpy as np
from jax import lax

D = 7168
TOP = 8
TOK_DEV = 16
FF = 1024
SFF = 1024
EXPERTS = 16
TOKENS = 256
CAP = 16
N_EP = 16


def block_levels(key, extent, split, low, largest):
    def one(dim, blocks):
        steps = jax.random.uniform(jax.random.fold_in(jax.random.fold_in(key, 6), dim), (blocks,), jnp.float32, low / len(split), largest / len(split))
        return jnp.repeat(jnp.exp(steps), extent[dim] // blocks).reshape((-1,) + (1,) * (len(extent) - dim - 1))

    factor_of = one(*split[0])
    for cut in split[1:]:
        factor_of = factor_of * one(*cut)
    return factor_of


def assign_block(key, own, number, rows, amount, top, most, lean):
    order = jax.random.permutation(key, amount)
    heavy_load, common = load_shares(amount, rows * top, most, lean, True), load_shares(amount, rows * top, most, lean, False)
    places = jnp.arange(amount)

    def named(sizes, offset_by):
        used = int((sizes > 0).sum())
        fixed = max(1, used // 4)
        passed = fixed + (places - fixed + offset_by * (used - fixed)) % max(1, amount - fixed)
        return jnp.zeros((amount,), jnp.int32).at[order[jnp.where(places < fixed, places, passed)]].set(jnp.asarray(sizes, jnp.int32))

    sizes = jnp.where(number % 4 == 0, named(heavy_load, number // 4), named(common, number - number // 4 - 1))
    mixed = jax.random.permutation(jax.random.fold_in(own, 3), amount)
    source_of, sink = mixed[0:amount // 2 * 2:2], mixed[1:amount // 2 * 2:2]
    room = jnp.minimum(sizes[source_of] - 1, most - sizes[sink]) // 2
    room = jnp.where((source_of == order[0]) | (sink == order[0]) | (sizes[sink] == 0), 0, jnp.maximum(room, 0))
    passed = jax.random.randint(jax.random.fold_in(own, 4), (amount // 2,), 0, 1 << 20) % (room + 1)
    sizes = sizes.at[source_of].add(-passed).at[sink].add(passed)
    items = jnp.searchsorted(jnp.cumsum(sizes), jnp.arange(rows * top), side="right").astype(jnp.int32)
    listing = items.reshape(top, rows).T
    listing = listing[jax.random.permutation(jax.random.fold_in(own, 1), rows)]
    offset_by = jax.random.randint(jax.random.fold_in(own, 2), (rows, 1), 0, top)
    return jnp.take_along_axis(listing, (jnp.arange(top)[None, :] + offset_by) % top, axis=1)


def load_shares(number_of, total, most, lean, full):
    loads = [(1 << 20) // math.isqrt(rank ** lean) + 1 for rank in range(1, number_of + 1)]
    largest = most if full else min(most, max(-(-total // number_of), total * loads[0] // sum(loads)))
    least = 1 if total - largest >= number_of - 1 else 0
    given, spare = [largest] + [least] * (number_of - 1), total - largest - least * (number_of - 1)
    while spare > 0:
        free = [i for i in range(1, number_of) if given[i] < largest] or [i for i in range(1, number_of) if given[i] < most]
        mass, left = sum([loads[i] for i in free]), spare
        for i in free:
            extra = min(most - given[i], max(1, left * loads[i] // mass), spare)
            given[i] = given[i] + extra
            spare = spare - extra
    return np.array(given)


def scatter_about(key, dims, deviation, most, pieces=(), kind=jnp.bfloat16):
    factor_of = block_levels(key, dims, pieces, -0.22, 0.18) if pieces else 1.0
    drawn = jax.random.normal(key, dims, jnp.float32) * deviation * factor_of
    return jnp.minimum(jnp.maximum(drawn, -most), most).astype(kind)


def setup_inputs(seed: int = 0) -> dict:
    streams_of = jax.random.split(jax.random.key(seed), 11)
    tokens = scatter_about(streams_of[0], (TOKENS, D), 1.0, 6.0, ((0, 16), (1, 2)))
    route_ids_keys = jax.random.split(jax.random.fold_in(streams_of[1], 1), TOKENS // TOK_DEV)
    route_ids_turns = jax.random.permutation(jax.random.fold_in(streams_of[1], 3), TOKENS // TOK_DEV)
    route_ids = jax.vmap(lambda own, number: assign_block(jax.random.fold_in(streams_of[1], 2), own, number, TOK_DEV, EXPERTS, TOP, CAP, 2))(route_ids_keys, route_ids_turns).reshape((TOKENS, TOP))
    expert_slot = jax.random.permutation(streams_of[2], EXPERTS).astype(jnp.int32)
    router_weight = scatter_about(streams_of[3], (D, EXPERTS), D ** -0.5, 0.0625, ((0, 2),))
    expert_gate = scatter_about(streams_of[4], (EXPERTS, D, FF), D ** -0.5, 0.0625, ((0, 16), (1, 2)))
    expert_up = scatter_about(streams_of[5], (EXPERTS, D, FF), D ** -0.5, 0.0625, ((0, 16), (1, 2)))
    expert_down = scatter_about(streams_of[6], (EXPERTS, FF, D), FF ** -0.5, 0.1875, ((0, 16), (2, 2)))
    shared_gate = scatter_about(streams_of[7], (D, SFF), D ** -0.5, 0.0625, ((0, 2), (1, 16)))
    shared_up = scatter_about(streams_of[8], (D, SFF), D ** -0.5, 0.0625, ((0, 2), (1, 16)))
    shared_down = scatter_about(streams_of[9], (SFF, D), SFF ** -0.5, 0.1875, ((0, 16), (1, 2)))
    return dict(tokens=tokens, route_ids=route_ids, expert_slot=expert_slot, router_weight=router_weight, expert_gate=expert_gate, expert_up=expert_up, expert_down=expert_down, shared_gate=shared_gate, shared_up=shared_up, shared_down=shared_down)


route_scale = 2.5


def reference(tokens, route_ids, expert_slot, router_weight, expert_gate, expert_up, expert_down, shared_gate, shared_up, shared_down):
    logits = jnp.dot(tokens, router_weight, preferred_element_type=jnp.float32)
    scores = jax.nn.sigmoid(logits)
    picked = jnp.take_along_axis(scores, route_ids, axis=1)
    gate_values = picked / jnp.sum(picked, axis=1, keepdims=True) * route_scale
    flat_ids = route_ids.reshape(-1).astype(jnp.int32)
    assignments = flat_ids.shape[0]
    onehot = (flat_ids[:, None] == jnp.arange(EXPERTS, dtype=jnp.int32)[None, :]).astype(jnp.int32)
    earlier = jnp.cumsum(onehot, axis=0) - onehot
    places = jnp.take_along_axis(earlier, flat_ids[:, None], axis=1)[:, 0].astype(jnp.int32)
    bucket = N_EP * CAP
    owners = jnp.arange(assignments, dtype=jnp.int32) // TOP
    token_table = jnp.full((EXPERTS, bucket), TOKENS, jnp.int32).at[flat_ids, places].set(owners)
    gate_table = jnp.zeros((EXPERTS, bucket), jnp.float32).at[flat_ids, places].set(gate_values.reshape(-1))
    zeros_row = jnp.zeros((1, D), tokens.dtype)
    padded = jnp.concatenate([tokens, zeros_row], axis=0)

    def expert_step(totals, expert):
        slot_index = expert_slot[expert]
        selected = padded[token_table[expert]]
        gate_part = jnp.dot(selected, expert_gate[slot_index], preferred_element_type=jnp.float32)
        up_part = jnp.dot(selected, expert_up[slot_index], preferred_element_type=jnp.float32)
        hidden = (jax.nn.silu(gate_part) * up_part).astype(jnp.bfloat16)
        produced = jnp.dot(hidden, expert_down[slot_index], preferred_element_type=jnp.float32).astype(jnp.bfloat16)
        weighted = produced.astype(jnp.float32) * gate_table[expert][:, None]
        totals = totals.at[token_table[expert]].add(weighted)
        return totals, None

    start_totals = jnp.zeros((TOKENS + 1, D), jnp.float32)
    totals, unused = lax.scan(expert_step, start_totals, jnp.arange(EXPERTS, dtype=jnp.int32))
    routed = totals[:TOKENS]
    shared_gate_part = jnp.dot(tokens, shared_gate, preferred_element_type=jnp.float32)
    shared_up_part = jnp.dot(tokens, shared_up, preferred_element_type=jnp.float32)
    shared_hidden = (jax.nn.silu(shared_gate_part) * shared_up_part).astype(jnp.bfloat16)
    shared_out = jnp.dot(shared_hidden, shared_down, preferred_element_type=jnp.float32)
    return (shared_out + routed).astype(jnp.bfloat16)
```

```python
import functools

import jax
import jax.numpy as jnp
from jax import lax
from jax.experimental import pallas as pl
from jax.experimental.pallas import tpu as pltpu
from jax.sharding import PartitionSpec as P
import math

route_scale = 2.5
MESH = pl.DeviceIdType.MESH


def silu(v):
    return v / (1.0 + jnp.exp(-v))


def dot(a, b):
    return jnp.dot(a, b, preferred_element_type=jnp.float32)


def kernel(
    n_ep,
    n_tp,
    chunks,
    tokens,
    ids,
    slot,
    rw_hbm,
    eg_hbm,
    eu_hbm,
    ed_hbm,
    sg_hbm,
    su_hbm,
    sd_hbm,
    out,
    x,
    wg,
    wu,
    wd,
    rw,
    sg,
    su,
    sw,
    sd,
    lg_part,
    lg_in,
    gates,
    gates_in,
    part,
    part_in,
    sh_part,
    sh_in,
    hid,
    hid_in,
    leave,
    arrive,
    w_sem,
    own_sem,
    x_send,
    x_recv,
    lg_send,
    lg_recv,
    ga_send,
    ga_recv,
    pa_send,
    pa_recv,
    sh_send,
    sh_recv,
    hi_send,
    hi_recv,
    le_send,
    le_recv,
):
    ep, tp = lax.axis_index("ep"), lax.axis_index("tp")
    rows, feats = tokens.shape
    experts = slot.shape[1]
    ff_part = wg.shape[2]
    sff = sg.shape[1]
    width = feats // chunks

    def ep_at(d):
        return lax.rem(ep + d, n_ep)

    def tp_at(d):
        return lax.rem(tp + d, n_tp)

    def row_block(ref, block):
        return ref.at[pl.ds(pl.multiple_of(block * rows, rows), rows), :]

    loads = [
        pltpu.make_async_copy(rw_hbm, rw, w_sem.at[0]),
        pltpu.make_async_copy(sg_hbm, sg, w_sem.at[1]),
        pltpu.make_async_copy(su_hbm, su, w_sem.at[2]),
        pltpu.make_async_copy(sd_hbm, sd, w_sem.at[3]),
        pltpu.make_async_copy(ed_hbm.at[0], wd, w_sem.at[4]),
    ]

    def piece_load(hbm, buf, j, sem):
        cols = pl.ds(pl.multiple_of(j * ff_part, ff_part), ff_part)
        return pltpu.make_async_copy(hbm.at[0, :, cols], buf.at[j], w_sem.at[sem + j])

    for load in loads[:3]:
        load.start()
    for j in range(n_tp):
        piece_load(eg_hbm, wg, j, 5).start()
        piece_load(eu_hbm, wu, j, 5 + n_tp).start()
    for load in loads[3:]:
        load.start()
    own = pltpu.make_async_copy(tokens, row_block(x, ep), own_sem.at[0])
    own.start()

    barrier = pltpu.get_barrier_semaphore()

    @pl.loop(1, n_ep)
    def _(d):
        pl.semaphore_signal(barrier, inc=1, device_id={"ep": ep_at(d)}, device_id_type=MESH)

    @pl.loop(1, n_tp)
    def _(d):
        pl.semaphore_signal(barrier, inc=1, device_id={"tp": tp_at(d)}, device_id_type=MESH)

    pl.semaphore_wait(barrier, n_ep + n_tp - 2)

    def token_copy(src, to):
        return pltpu.make_async_remote_copy(
            src_ref=tokens,
            dst_ref=row_block(x, src),
            send_sem=x_send.at[to],
            recv_sem=x_recv.at[src],
            device_id={"ep": to},
            device_id_type=MESH,
        )

    @pl.loop(1, n_ep)
    def _(d):
        token_copy(ep, ep_at(d)).start()

    def to_tp(src_ref, in_ref, send, recv, slot_in, to):
        return pltpu.make_async_remote_copy(
            src_ref=src_ref,
            dst_ref=in_ref.at[slot_in],
            send_sem=send.at[to],
            recv_sem=recv.at[slot_in],
            device_id={"tp": to},
            device_id_type=MESH,
        )

    loads[0].wait()
    lg_part[...] = dot(tokens[...], rw[...])
    lg_in[tp] = lg_part[...]

    @pl.loop(1, n_tp)
    def _(d):
        to_tp(lg_part, lg_in, lg_send, lg_recv, tp, tp_at(d)).start()

    loads[1].wait()
    loads[2].wait()
    sw[:, 0:sff] = sg[...]
    sw[:, sff : 2 * sff] = su[...]

    @pl.loop(1, n_tp)
    def _(d):
        to_tp(lg_part, lg_in, lg_send, lg_recv, tp_at(d), tp_at(d)).wait()

    logits = lg_in[0]
    for j in range(1, n_tp):
        logits = logits + lg_in[j]
    expert_iota = lax.broadcasted_iota(jnp.int32, (rows, experts), 1)
    mask = jnp.zeros((rows, experts), jnp.float32)
    for k in range(ids.shape[1]):
        mask = mask + jnp.where(ids[:, k : k + 1] == expert_iota, 1.0, 0.0)
    picked = mask * (1.0 / (1.0 + jnp.exp(-logits)))
    gates[...] = picked / jnp.sum(picked, axis=1, keepdims=True) * route_scale
    gates_in[pl.ds(pl.multiple_of(ep * rows, rows), rows), :] = gates[...]

    def gate_copy(src, to):
        return pltpu.make_async_remote_copy(
            src_ref=gates,
            dst_ref=row_block(gates_in, src),
            send_sem=ga_send.at[to],
            recv_sem=ga_recv.at[src],
            device_id={"ep": to},
            device_id_type=MESH,
        )

    @pl.loop(1, n_ep)
    def _(d):
        gate_copy(ep, ep_at(d)).start()

    own.wait()

    @pl.loop(1, n_ep)
    def _(d):
        token_copy(ep_at(d), ep_at(d)).wait()

    def gate_up(j):
        piece_load(eg_hbm, wg, j, 5).wait()
        piece_load(eu_hbm, wu, j, 5 + n_tp).wait()
        part[j, 0] = dot(x[...], wg[j])
        part[j, 1] = dot(x[...], wu[j])

    @pl.loop(1, n_tp)
    def _(d):
        j = tp_at(d)
        gate_up(j)
        to_tp(part.at[j], part_in, pa_send, pa_recv, tp, j).start()

    sh_part[...] = dot(x[...], sw[...])

    @pl.loop(1, n_tp)
    def _(d):
        to_tp(sh_part, sh_in, sh_send, sh_recv, tp, tp_at(d)).start()

    gate_up(tp)

    @pl.loop(1, n_tp)
    def _(d):
        j = tp_at(d)
        to_tp(part.at[j], part_in, pa_send, pa_recv, j, j).wait()

    @pl.loop(1, n_tp)
    def _(d):
        j = tp_at(d)
        part[tp] = part[tp] + part_in[j]

    hid[...] = (silu(part[tp, 0]) * part[tp, 1]).astype(jnp.bfloat16)
    hid_in[tp] = hid[...]

    @pl.loop(1, n_tp)
    def _(d):
        to_tp(hid, hid_in, hi_send, hi_recv, tp, tp_at(d)).start()

    @pl.loop(1, n_tp)
    def _(d):
        j = tp_at(d)
        to_tp(sh_part, sh_in, sh_send, sh_recv, j, j).wait()

    sh_in[tp] = sh_part[...]
    sh_sum = sh_in[0]
    for j in range(1, n_tp):
        sh_sum = sh_sum + sh_in[j]
    sh_hid = (silu(sh_sum[:, 0:sff]) * sh_sum[:, sff : 2 * sff]).astype(jnp.bfloat16)

    @pl.loop(1, n_ep)
    def _(d):
        gate_copy(ep_at(d), ep_at(d)).wait()

    mine = jnp.where(slot[...] == ep, 1.0, 0.0)
    column = jnp.sum(gates_in[...] * mine, axis=1, keepdims=True)

    loads[3].wait()
    loads[4].wait()

    @pl.loop(1, n_tp)
    def _(d):
        j = tp_at(d)
        to_tp(hid, hid_in, hi_send, hi_recv, j, j).wait()

    def leave_copy(chunk, src, to):
        return pltpu.make_async_remote_copy(
            src_ref=row_block(leave.at[chunk], to),
            dst_ref=row_block(arrive.at[chunk], src),
            send_sem=le_send.at[chunk, to],
            recv_sem=le_recv.at[chunk, src],
            device_id={"ep": to},
            device_id_type=MESH,
        )

    @pl.loop(0, chunks)
    def _(chunk):
        cols = pl.ds(pl.multiple_of(chunk * width, width), width)
        total = dot(hid_in[0], wd[0:ff_part, cols])
        for j in range(1, n_tp):
            total = total + dot(hid_in[j], wd[j * ff_part : (j + 1) * ff_part, cols])
        given = total.astype(jnp.bfloat16).astype(jnp.float32) * column
        given = given + dot(sh_hid, sd[:, cols])
        leave[chunk] = given.astype(jnp.bfloat16)

        @pl.loop(1, n_ep)
        def _(d):
            leave_copy(chunk, ep, ep_at(d)).start()

    @pl.loop(0, chunks)
    def _(chunk):
        cols = pl.ds(pl.multiple_of(chunk * width, width), width)
        here = pl.ds(pl.multiple_of(ep * rows, rows), rows)
        arrive[chunk, here, :] = leave[chunk, here, :]

        @pl.loop(1, n_ep)
        def _(d):
            leave_copy(chunk, ep_at(d), ep_at(d)).wait()

        def add(src, total):
            block = arrive[chunk, pl.ds(pl.multiple_of(src * rows, rows), rows), :]
            return total + block.astype(jnp.float32)

        total = lax.fori_loop(0, n_ep, add, jnp.zeros((rows, width), jnp.float32))
        out[:, cols] = total.astype(jnp.bfloat16)


def on_device(n_ep, n_tp, *args):
    (tokens, ids, slot, rw, eg, eu, ed, sg, su, sd) = args
    rows, feats = tokens.shape
    experts = slot.shape[0]
    ff = eg.shape[2]
    sff = sg.shape[1]
    everyone = rows * n_ep
    ff_part = ff // n_tp
    chunks = math.gcd(feats // 128, 4)
    width = feats // chunks
    bf, f32 = jnp.bfloat16, jnp.float32
    dma = pltpu.SemaphoreType.DMA
    vmem = pl.BlockSpec(memory_space=pltpu.VMEM)
    hbm = pl.BlockSpec(memory_space=pl.ANY)
    return pl.pallas_call(
        functools.partial(kernel, n_ep, n_tp, chunks),
        out_shape=jax.ShapeDtypeStruct((rows, feats), bf),
        in_specs=[vmem] * 3 + [hbm] * 7,
        out_specs=vmem,
        scratch_shapes=[
            pltpu.VMEM((everyone, feats), bf),
            pltpu.VMEM((n_tp, feats, ff_part), bf),
            pltpu.VMEM((n_tp, feats, ff_part), bf),
            pltpu.VMEM((ff, feats), bf),
            pltpu.VMEM((feats, experts), bf),
            pltpu.VMEM((feats, sff), bf),
            pltpu.VMEM((feats, sff), bf),
            pltpu.VMEM((feats, 2 * sff), bf),
            pltpu.VMEM((sff, feats), bf),
            pltpu.VMEM((rows, experts), f32),
            pltpu.VMEM((n_tp, rows, experts), f32),
            pltpu.VMEM((rows, experts), f32),
            pltpu.VMEM((everyone, experts), f32),
            pltpu.VMEM((n_tp, 2, everyone, ff_part), f32),
            pltpu.VMEM((n_tp, 2, everyone, ff_part), f32),
            pltpu.VMEM((everyone, 2 * sff), f32),
            pltpu.VMEM((n_tp, everyone, 2 * sff), f32),
            pltpu.VMEM((everyone, ff_part), bf),
            pltpu.VMEM((n_tp, everyone, ff_part), bf),
            pltpu.VMEM((chunks, everyone, width), bf),
            pltpu.VMEM((chunks, everyone, width), bf),
            dma((5 + 2 * n_tp,)),
            dma((1,)),
            dma((n_ep,)),
            dma((n_ep,)),
            dma((n_tp,)),
            dma((n_tp,)),
            dma((n_ep,)),
            dma((n_ep,)),
            dma((n_tp,)),
            dma((n_tp,)),
            dma((n_tp,)),
            dma((n_tp,)),
            dma((n_tp,)),
            dma((n_tp,)),
            dma((chunks, n_ep)),
            dma((chunks, n_ep)),
        ],
        compiler_params=pltpu.CompilerParams(
            collective_id=0, has_side_effects=True, vmem_limit_bytes=63 * 1024 * 1024
        ),
    )(tokens, ids, slot[None, :], rw, eg, eu, ed, sg, su, sd)


def solution(mesh):
    placed = (
        P("ep", "tp"),
        P("ep", None),
        P(),
        P("tp", None),
        P("ep", "tp", None),
        P("ep", "tp", None),
        P("ep", None, "tp"),
        P("tp", "ep"),
        P("tp", "ep"),
        P("ep", "tp"),
    )
    return jax.shard_map(
        functools.partial(on_device, mesh.shape["ep"], mesh.shape["tp"]),
        mesh=mesh,
        in_specs=placed,
        out_specs=P("ep", "tp"),
        check_vma=False,
    )
```

```python
import functools

import jax
import jax.numpy as jnp
from jax import lax
from jax.experimental import pallas as pl
from jax.experimental.pallas import tpu as pltpu
from jax.sharding import PartitionSpec as P
import math

route_scale = 2.5
MESH = pl.DeviceIdType.MESH


def silu(v):
    return v / (1.0 + jnp.exp(-v))


def dot(a, b):
    return jnp.dot(a, b, preferred_element_type=jnp.float32)


def dot_t(a, b):
    return lax.dot_general(a, b, (((1,), (1,)), ((), ())), preferred_element_type=jnp.float32)


def kernel(
    n_ep,
    n_tp,
    chunks,
    tokens,
    ids,
    slot,
    rw_hbm,
    eg_hbm,
    eu_hbm,
    ed_hbm,
    sg_hbm,
    su_hbm,
    sd_hbm,
    out,
    x,
    wg,
    wu,
    wd,
    sw,
    sd,
    lg_part,
    lg_in,
    gates,
    gates_in,
    part,
    part_in,
    sh_part,
    sh_in,
    hid,
    hid_in,
    leave,
    arrive,
    w_sem,
    own_sem,
    x_send,
    x_recv,
    lg_send,
    lg_recv,
    ga_send,
    ga_recv,
    pa_send,
    pa_recv,
    sh_send,
    sh_recv,
    hi_send,
    hi_recv,
    le_send,
    le_recv,
):
    ep, tp = lax.axis_index("ep"), lax.axis_index("tp")
    rows, feats = tokens.shape
    experts = slot.shape[1]
    ff_part = wg.shape[2]
    sff = sg_hbm.shape[0]
    width = feats // chunks

    def ep_at(d):
        return lax.rem(ep + d, n_ep)

    def tp_at(d):
        return lax.rem(tp + d, n_tp)

    def row_block(ref, block):
        return ref.at[pl.ds(pl.multiple_of(block * rows, rows), rows), :]

    loads = [
        pltpu.make_async_copy(rw_hbm, sw.at[2 * sff : 2 * sff + experts, :], w_sem.at[0]),
        pltpu.make_async_copy(sg_hbm, sw.at[0:sff, :], w_sem.at[1]),
        pltpu.make_async_copy(su_hbm, sw.at[sff : 2 * sff, :], w_sem.at[2]),
        pltpu.make_async_copy(sd_hbm, sd, w_sem.at[3]),
        pltpu.make_async_copy(ed_hbm.at[0], wd, w_sem.at[4]),
    ]

    def piece_load(hbm, buf, j, sem):
        cols = pl.ds(pl.multiple_of(j * ff_part, ff_part), ff_part)
        return pltpu.make_async_copy(hbm.at[0, :, cols], buf.at[j], w_sem.at[sem + j])

    for load in loads[:3]:
        load.start()
    for j in range(n_tp):
        piece_load(eg_hbm, wg, j, 5).start()
        piece_load(eu_hbm, wu, j, 5 + n_tp).start()
    for load in loads[3:]:
        load.start()
    own = pltpu.make_async_copy(tokens, row_block(x, ep), own_sem.at[0])
    own.start()

    barrier = pltpu.get_barrier_semaphore()

    @pl.loop(1, n_ep)
    def _(d):
        pl.semaphore_signal(barrier, inc=1, device_id={"ep": ep_at(d)}, device_id_type=MESH)

    @pl.loop(1, n_tp)
    def _(d):
        pl.semaphore_signal(barrier, inc=1, device_id={"tp": tp_at(d)}, device_id_type=MESH)

    pl.semaphore_wait(barrier, n_ep + n_tp - 2)

    near = 1 + lax.rem(tp, 2)
    far = 3 - near
    line = n_ep // 4
    level = ep // 4
    near_bit, far_bit = lax.rem(ep // near, 2), lax.rem(ep // far, 2)
    near_peer = ep + near * (1 - 2 * near_bit)
    far_peer = ep + far * (1 - 2 * far_bit)

    def token_copy(way, src, to, src_ref=None):
        return pltpu.make_async_remote_copy(
            src_ref=row_block(x, src) if src_ref is None else src_ref,
            dst_ref=row_block(x, src),
            send_sem=x_send.at[way, src],
            recv_sem=x_recv.at[src],
            device_id={"ep": to},
            device_id_type=MESH,
        )

    def pass_on(src, up, down, src_ref=None):
        @pl.when(up)
        def _():
            token_copy(0, src, lax.rem(ep + 4, n_ep), src_ref).start()

        @pl.when(down)
        def _():
            token_copy(1, src, lax.rem(ep + n_ep - 4, n_ep), src_ref).start()

        token_copy(2, src, far_peer, src_ref).start()

    can_up, can_down = level < line - 1, level > 0
    token_copy(3, ep, near_peer, tokens).start()
    pass_on(ep, can_up, can_down, tokens)

    token_copy(3, near_peer, near_peer).wait_recv()
    pass_on(near_peer, can_up, can_down)

    @pl.loop(1, line)
    def _(far_off):
        for side in (ep, near_peer):
            below, above = side - 4 * far_off, side + 4 * far_off

            @pl.when(level >= far_off)
            def _():
                token_copy(0, below, ep).wait_recv()
                pass_on(below, can_up, False)

            @pl.when(level + far_off < line)
            def _():
                token_copy(1, above, ep).wait_recv()
                pass_on(above, False, can_down)

    def to_tp(src_ref, in_ref, send, recv, slot_in, to):
        return pltpu.make_async_remote_copy(
            src_ref=src_ref,
            dst_ref=in_ref.at[slot_in],
            send_sem=send.at[to],
            recv_sem=recv.at[slot_in],
            device_id={"tp": to},
            device_id_type=MESH,
        )

    loads[0].wait()
    lg_part[...] = dot_t(tokens[...], sw[2 * sff : 2 * sff + experts, :])
    lg_in[tp] = lg_part[...]

    @pl.loop(1, n_tp)
    def _(d):
        to_tp(lg_part, lg_in, lg_send, lg_recv, tp, tp_at(d)).start()

    @pl.loop(1, n_tp)
    def _(d):
        to_tp(lg_part, lg_in, lg_send, lg_recv, tp_at(d), tp_at(d)).wait()

    logits = lg_in[0]
    for j in range(1, n_tp):
        logits = logits + lg_in[j]
    turned_iota = lax.broadcasted_iota(jnp.int32, (experts, rows), 0)
    turned = jnp.zeros((experts, rows), jnp.float32)
    for k in range(ids.shape[0]):
        turned = turned + jnp.where(ids[k : k + 1, :] == turned_iota, 1.0, 0.0)
    row_iota = lax.broadcasted_iota(jnp.int32, (rows, rows), 0)
    same = row_iota == lax.broadcasted_iota(jnp.int32, (rows, rows), 1)
    eye = jnp.where(same, 1.0, 0.0).astype(jnp.bfloat16)
    mask = dot_t(eye, turned.astype(jnp.bfloat16))
    picked = mask * (1.0 / (1.0 + jnp.exp(-logits)))
    gates[...] = picked / jnp.sum(picked, axis=1, keepdims=True) * route_scale
    gates_in[pl.ds(pl.multiple_of(ep * rows, rows), rows), :] = gates[...]

    def gate_copy(src, to):
        return pltpu.make_async_remote_copy(
            src_ref=gates,
            dst_ref=row_block(gates_in, src),
            send_sem=ga_send.at[to],
            recv_sem=ga_recv.at[src],
            device_id={"ep": to},
            device_id_type=MESH,
        )

    @pl.loop(1, n_ep)
    def _(d):
        gate_copy(ep, ep_at(d)).start()

    own.wait()

    @pl.loop(0, line)
    def _(at):
        for side in (ep, near_peer):
            mine_there = lax.rem(side, 4) + 4 * at
            token_copy(2, mine_there + far * (1 - 2 * far_bit), ep).wait_recv()
            token_copy(2, mine_there, far_peer).wait_send()

            @pl.when(can_up & (at <= level))
            def _():
                token_copy(0, mine_there, ep).wait_send()

            @pl.when(can_down & (at >= level))
            def _():
                token_copy(1, mine_there, ep).wait_send()

    token_copy(3, ep, near_peer).wait_send()

    def gate_up(j):
        piece_load(eg_hbm, wg, j, 5).wait()
        piece_load(eu_hbm, wu, j, 5 + n_tp).wait()
        part[j, 0] = dot(x[...], wg[j])
        part[j, 1] = dot(x[...], wu[j])

    @pl.loop(1, n_tp)
    def _(d):
        j = tp_at(d)
        gate_up(j)
        to_tp(part.at[j], part_in, pa_send, pa_recv, tp, j).start()

    loads[1].wait()
    loads[2].wait()
    sh_part[...] = dot_t(x[...], sw[0 : 2 * sff, :])

    @pl.loop(1, n_tp)
    def _(d):
        to_tp(sh_part, sh_in, sh_send, sh_recv, tp, tp_at(d)).start()

    gate_up(tp)

    @pl.loop(1, n_tp)
    def _(d):
        j = tp_at(d)
        to_tp(part.at[j], part_in, pa_send, pa_recv, j, j).wait()

    @pl.loop(1, n_tp)
    def _(d):
        j = tp_at(d)
        part[tp] = part[tp] + part_in[j]

    hid[...] = (silu(part[tp, 0]) * part[tp, 1]).astype(jnp.bfloat16)
    hid_in[tp] = hid[...]

    @pl.loop(1, n_tp)
    def _(d):
        to_tp(hid, hid_in, hi_send, hi_recv, tp, tp_at(d)).start()

    @pl.loop(1, n_tp)
    def _(d):
        j = tp_at(d)
        to_tp(sh_part, sh_in, sh_send, sh_recv, j, j).wait()

    sh_in[tp] = sh_part[...]
    sh_sum = sh_in[0]
    for j in range(1, n_tp):
        sh_sum = sh_sum + sh_in[j]
    sh_hid = (silu(sh_sum[:, 0:sff]) * sh_sum[:, sff : 2 * sff]).astype(jnp.bfloat16)

    @pl.loop(1, n_ep)
    def _(d):
        gate_copy(ep_at(d), ep_at(d)).wait()

    mine = jnp.where(slot[...] == ep, 1.0, 0.0)
    column = jnp.sum(gates_in[...] * mine, axis=1, keepdims=True)

    loads[3].wait()
    loads[4].wait()

    @pl.loop(1, n_tp)
    def _(d):
        j = tp_at(d)
        to_tp(hid, hid_in, hi_send, hi_recv, j, j).wait()

    def leave_copy(chunk, src, to):
        return pltpu.make_async_remote_copy(
            src_ref=row_block(leave.at[chunk], to),
            dst_ref=row_block(arrive.at[chunk], src),
            send_sem=le_send.at[chunk, to],
            recv_sem=le_recv.at[chunk, src],
            device_id={"ep": to},
            device_id_type=MESH,
        )

    @pl.loop(0, chunks)
    def _(chunk):
        cols = pl.ds(pl.multiple_of(chunk * width, width), width)
        total = dot(hid_in[0], wd[0:ff_part, cols])
        for j in range(1, n_tp):
            total = total + dot(hid_in[j], wd[j * ff_part : (j + 1) * ff_part, cols])
        given = total.astype(jnp.bfloat16).astype(jnp.float32) * column
        given = given + dot(sh_hid, sd[:, cols])
        leave[chunk] = given.astype(jnp.bfloat16)

        @pl.loop(1, n_ep)
        def _(d):
            leave_copy(chunk, ep, ep_at(d)).start()

    @pl.loop(0, chunks)
    def _(chunk):
        cols = pl.ds(pl.multiple_of(chunk * width, width), width)
        here = pl.ds(pl.multiple_of(ep * rows, rows), rows)
        arrive[chunk, here, :] = leave[chunk, here, :]

        @pl.loop(1, n_ep)
        def _(d):
            leave_copy(chunk, ep_at(d), ep_at(d)).wait()

        def add(src, total):
            block = arrive[chunk, pl.ds(pl.multiple_of(src * rows, rows), rows), :]
            return total + block.astype(jnp.float32)

        total = lax.fori_loop(0, n_ep, add, jnp.zeros((rows, width), jnp.float32))
        out[:, cols] = total.astype(jnp.bfloat16)


def on_device(n_ep, n_tp, *args):
    (tokens, ids, slot, rw, eg, eu, ed, sg, su, sd) = args
    rows, feats = tokens.shape
    experts = slot.shape[0]
    ff = eg.shape[2]
    sff = sg.shape[1]
    assert n_ep % 4 == 0
    everyone = rows * n_ep
    ff_part = ff // n_tp
    chunks = math.gcd(feats // 128, 4)
    width = feats // chunks
    bf, f32 = jnp.bfloat16, jnp.float32
    dma = pltpu.SemaphoreType.DMA
    vmem = pl.BlockSpec(memory_space=pltpu.VMEM)
    hbm = pl.BlockSpec(memory_space=pl.ANY)
    return pl.pallas_call(
        functools.partial(kernel, n_ep, n_tp, chunks),
        out_shape=jax.ShapeDtypeStruct((rows, feats), bf),
        in_specs=[vmem] * 3 + [hbm] * 7,
        out_specs=vmem,
        scratch_shapes=[
            pltpu.VMEM((everyone, feats), bf),
            pltpu.VMEM((n_tp, feats, ff_part), bf),
            pltpu.VMEM((n_tp, feats, ff_part), bf),
            pltpu.VMEM((ff, feats), bf),
            pltpu.VMEM((2 * sff + experts, feats), bf),
            pltpu.VMEM((sff, feats), bf),
            pltpu.VMEM((rows, experts), f32),
            pltpu.VMEM((n_tp, rows, experts), f32),
            pltpu.VMEM((rows, experts), f32),
            pltpu.VMEM((everyone, experts), f32),
            pltpu.VMEM((n_tp, 2, everyone, ff_part), f32),
            pltpu.VMEM((n_tp, 2, everyone, ff_part), f32),
            pltpu.VMEM((everyone, 2 * sff), f32),
            pltpu.VMEM((n_tp, everyone, 2 * sff), f32),
            pltpu.VMEM((everyone, ff_part), bf),
            pltpu.VMEM((n_tp, everyone, ff_part), bf),
            pltpu.VMEM((chunks, everyone, width), bf),
            pltpu.VMEM((chunks, everyone, width), bf),
            dma((5 + 2 * n_tp,)),
            dma((1,)),
            dma((4, n_ep)),
            dma((n_ep,)),
            dma((n_tp,)),
            dma((n_tp,)),
            dma((n_ep,)),
            dma((n_ep,)),
            dma((n_tp,)),
            dma((n_tp,)),
            dma((n_tp,)),
            dma((n_tp,)),
            dma((n_tp,)),
            dma((n_tp,)),
            dma((chunks, n_ep)),
            dma((chunks, n_ep)),
        ],
        compiler_params=pltpu.CompilerParams(
            collective_id=0, has_side_effects=True, vmem_limit_bytes=63 * 1024 * 1024
        ),
    )(tokens, ids.T, slot[None, :], rw.T, eg, eu, ed, sg.T, su.T, sd)


def solution(mesh):
    placed = (
        P("ep", "tp"),
        P("ep", None),
        P(),
        P("tp", None),
        P("ep", "tp", None),
        P("ep", "tp", None),
        P("ep", None, "tp"),
        P("tp", "ep"),
        P("tp", "ep"),
        P("ep", "tp"),
    )
    return jax.shard_map(
        functools.partial(on_device, mesh.shape["ep"], mesh.shape["tp"]),
        mesh=mesh,
        in_specs=placed,
        out_specs=P("ep", "tp"),
        check_vma=False,
    )
```

```python
import functools

import jax
import jax.numpy as jnp
from jax import lax
from jax.experimental import pallas as pl
from jax.experimental.pallas import tpu as pltpu
from jax.sharding import PartitionSpec as P
import math

route_scale = 2.5
MESH = pl.DeviceIdType.MESH


def silu(v):
    return v / (1.0 + jnp.exp(-v))


def dot(a, b):
    return jnp.dot(a, b, preferred_element_type=jnp.float32)


def dot_t(a, b):
    return lax.dot_general(a, b, (((1,), (1,)), ((), ())), preferred_element_type=jnp.float32)


def kernel(
    n_ep,
    n_tp,
    chunks,
    tokens,
    ids,
    slot,
    rw_hbm,
    eg_hbm,
    eu_hbm,
    ed_hbm,
    sg_hbm,
    su_hbm,
    sd_hbm,
    out,
    x,
    wg,
    wu,
    wd,
    sw,
    sd,
    lg_part,
    lg_in,
    gates,
    gates_in,
    part,
    part_in,
    sh_part,
    sh_in,
    hid,
    hid_in,
    whole,
    keep,
    leave_far,
    come_far,
    leave_line,
    come_line,
    leave_near,
    come_near,
    w_sem,
    own_sem,
    x_send,
    x_recv,
    lg_send,
    lg_recv,
    ga_send,
    ga_recv,
    pa_send,
    pa_recv,
    sh_send,
    sh_recv,
    hi_send,
    hi_recv,
    far_send,
    far_recv,
    line_send,
    line_recv,
    near_send,
    near_recv,
):
    ep, tp = lax.axis_index("ep"), lax.axis_index("tp")
    rows, feats = tokens.shape
    experts = slot.shape[1]
    ff_part = wg.shape[2]
    sff = sg_hbm.shape[0]
    width = feats // chunks

    def ep_at(d):
        return lax.rem(ep + d, n_ep)

    def tp_at(d):
        return lax.rem(tp + d, n_tp)

    def row_block(ref, block):
        return ref.at[pl.ds(pl.multiple_of(block * rows, rows), rows), :]

    loads = [
        pltpu.make_async_copy(rw_hbm, sw.at[2 * sff : 2 * sff + experts, :], w_sem.at[0]),
        pltpu.make_async_copy(sg_hbm, sw.at[0:sff, :], w_sem.at[1]),
        pltpu.make_async_copy(su_hbm, sw.at[sff : 2 * sff, :], w_sem.at[2]),
        pltpu.make_async_copy(sd_hbm, sd, w_sem.at[3]),
        pltpu.make_async_copy(ed_hbm.at[0], wd, w_sem.at[4]),
    ]

    def piece_load(hbm, buf, j, sem):
        cols = pl.ds(pl.multiple_of(j * ff_part, ff_part), ff_part)
        return pltpu.make_async_copy(hbm.at[0, :, cols], buf.at[j], w_sem.at[sem + j])

    for load in loads[:3]:
        load.start()
    for j in range(n_tp):
        piece_load(eg_hbm, wg, j, 5).start()
        piece_load(eu_hbm, wu, j, 5 + n_tp).start()
    for load in loads[3:]:
        load.start()
    own = pltpu.make_async_copy(tokens, row_block(x, ep), own_sem.at[0])
    own.start()

    barrier = pltpu.get_barrier_semaphore()

    @pl.loop(1, n_ep)
    def _(d):
        pl.semaphore_signal(barrier, inc=1, device_id={"ep": ep_at(d)}, device_id_type=MESH)

    @pl.loop(1, n_tp)
    def _(d):
        pl.semaphore_signal(barrier, inc=1, device_id={"tp": tp_at(d)}, device_id_type=MESH)

    pl.semaphore_wait(barrier, n_ep + n_tp - 2)

    near = 1 + lax.rem(tp, 2)
    far = 3 - near
    line = n_ep // 4
    level = ep // 4
    near_bit, far_bit = lax.rem(ep // near, 2), lax.rem(ep // far, 2)
    near_peer = ep + near * (1 - 2 * near_bit)
    far_peer = ep + far * (1 - 2 * far_bit)

    def token_copy(way, src, to, src_ref=None):
        return pltpu.make_async_remote_copy(
            src_ref=row_block(x, src) if src_ref is None else src_ref,
            dst_ref=row_block(x, src),
            send_sem=x_send.at[way, src],
            recv_sem=x_recv.at[src],
            device_id={"ep": to},
            device_id_type=MESH,
        )

    def pass_on(src, up, down, src_ref=None):
        @pl.when(up)
        def _():
            token_copy(0, src, lax.rem(ep + 4, n_ep), src_ref).start()

        @pl.when(down)
        def _():
            token_copy(1, src, lax.rem(ep + n_ep - 4, n_ep), src_ref).start()

        token_copy(2, src, far_peer, src_ref).start()

    can_up, can_down = level < line - 1, level > 0
    token_copy(3, ep, near_peer, tokens).start()
    pass_on(ep, can_up, can_down, tokens)

    token_copy(3, near_peer, near_peer).wait_recv()
    pass_on(near_peer, can_up, can_down)

    @pl.loop(1, line)
    def _(far_off):
        for side in (ep, near_peer):
            below, above = side - 4 * far_off, side + 4 * far_off

            @pl.when(level >= far_off)
            def _():
                token_copy(0, below, ep).wait_recv()
                pass_on(below, can_up, False)

            @pl.when(level + far_off < line)
            def _():
                token_copy(1, above, ep).wait_recv()
                pass_on(above, False, can_down)

    def to_tp(src_ref, in_ref, send, recv, slot_in, to):
        return pltpu.make_async_remote_copy(
            src_ref=src_ref,
            dst_ref=in_ref.at[slot_in],
            send_sem=send.at[to],
            recv_sem=recv.at[slot_in],
            device_id={"tp": to},
            device_id_type=MESH,
        )

    loads[0].wait()
    lg_part[...] = dot_t(tokens[...], sw[2 * sff : 2 * sff + experts, :])
    lg_in[tp] = lg_part[...]

    @pl.loop(1, n_tp)
    def _(d):
        to_tp(lg_part, lg_in, lg_send, lg_recv, tp, tp_at(d)).start()

    @pl.loop(1, n_tp)
    def _(d):
        to_tp(lg_part, lg_in, lg_send, lg_recv, tp_at(d), tp_at(d)).wait()

    logits = lg_in[0]
    for j in range(1, n_tp):
        logits = logits + lg_in[j]
    turned_iota = lax.broadcasted_iota(jnp.int32, (experts, rows), 0)
    turned = jnp.zeros((experts, rows), jnp.float32)
    for k in range(ids.shape[0]):
        turned = turned + jnp.where(ids[k : k + 1, :] == turned_iota, 1.0, 0.0)
    row_iota = lax.broadcasted_iota(jnp.int32, (rows, rows), 0)
    same = row_iota == lax.broadcasted_iota(jnp.int32, (rows, rows), 1)
    eye = jnp.where(same, 1.0, 0.0).astype(jnp.bfloat16)
    mask = dot_t(eye, turned.astype(jnp.bfloat16))
    picked = mask * (1.0 / (1.0 + jnp.exp(-logits)))
    gates[...] = picked / jnp.sum(picked, axis=1, keepdims=True) * route_scale
    gates_in[pl.ds(pl.multiple_of(ep * rows, rows), rows), :] = gates[...]

    def gate_copy(src, to):
        return pltpu.make_async_remote_copy(
            src_ref=gates,
            dst_ref=row_block(gates_in, src),
            send_sem=ga_send.at[to],
            recv_sem=ga_recv.at[src],
            device_id={"ep": to},
            device_id_type=MESH,
        )

    @pl.loop(1, n_ep)
    def _(d):
        gate_copy(ep, ep_at(d)).start()

    own.wait()

    @pl.loop(0, line)
    def _(at):
        for side in (ep, near_peer):
            mine_there = lax.rem(side, 4) + 4 * at
            token_copy(2, mine_there + far * (1 - 2 * far_bit), ep).wait_recv()
            token_copy(2, mine_there, far_peer).wait_send()

            @pl.when(can_up & (at <= level))
            def _():
                token_copy(0, mine_there, ep).wait_send()

            @pl.when(can_down & (at >= level))
            def _():
                token_copy(1, mine_there, ep).wait_send()

    token_copy(3, ep, near_peer).wait_send()

    def gate_up(j):
        piece_load(eg_hbm, wg, j, 5).wait()
        piece_load(eu_hbm, wu, j, 5 + n_tp).wait()
        part[j, 0] = dot(x[...], wg[j])
        part[j, 1] = dot(x[...], wu[j])

    @pl.loop(1, n_tp)
    def _(d):
        j = tp_at(d)
        gate_up(j)
        to_tp(part.at[j], part_in, pa_send, pa_recv, tp, j).start()

    loads[1].wait()
    loads[2].wait()
    sh_part[...] = dot_t(x[...], sw[0 : 2 * sff, :])

    @pl.loop(1, n_tp)
    def _(d):
        to_tp(sh_part, sh_in, sh_send, sh_recv, tp, tp_at(d)).start()

    gate_up(tp)

    @pl.loop(1, n_tp)
    def _(d):
        j = tp_at(d)
        to_tp(part.at[j], part_in, pa_send, pa_recv, j, j).wait()

    @pl.loop(1, n_tp)
    def _(d):
        j = tp_at(d)
        part[tp] = part[tp] + part_in[j]

    hid[...] = (silu(part[tp, 0]) * part[tp, 1]).astype(jnp.bfloat16)
    hid_in[tp] = hid[...]

    @pl.loop(1, n_tp)
    def _(d):
        to_tp(hid, hid_in, hi_send, hi_recv, tp, tp_at(d)).start()

    @pl.loop(1, n_tp)
    def _(d):
        j = tp_at(d)
        to_tp(sh_part, sh_in, sh_send, sh_recv, j, j).wait()

    sh_in[tp] = sh_part[...]
    sh_sum = sh_in[0]
    for j in range(1, n_tp):
        sh_sum = sh_sum + sh_in[j]
    sh_hid = (silu(sh_sum[:, 0:sff]) * sh_sum[:, sff : 2 * sff]).astype(jnp.bfloat16)

    @pl.loop(1, n_ep)
    def _(d):
        gate_copy(ep_at(d), ep_at(d)).wait()

    mine = jnp.where(slot[...] == ep, 1.0, 0.0)
    column = jnp.sum(gates_in[...] * mine, axis=1, keepdims=True)

    loads[3].wait()
    loads[4].wait()

    @pl.loop(1, n_tp)
    def _(d):
        j = tp_at(d)
        to_tp(hid, hid_in, hi_send, hi_recv, j, j).wait()

    half = 2 * line
    pair = 2 * rows
    here = pl.ds(pl.multiple_of(level * pair, pair), pair)

    def far_copy(chunk):
        return pltpu.make_async_remote_copy(
            src_ref=leave_far.at[chunk],
            dst_ref=come_far.at[chunk],
            send_sem=far_send.at[chunk],
            recv_sem=far_recv.at[chunk],
            device_id={"ep": far_peer},
            device_id_type=MESH,
        )

    def line_copy(chunk, src, to):
        return pltpu.make_async_remote_copy(
            src_ref=leave_line.at[chunk, pl.ds(pl.multiple_of(to * pair, pair), pair), :],
            dst_ref=come_line.at[chunk, pl.ds(pl.multiple_of(src * pair, pair), pair), :],
            send_sem=line_send.at[chunk, to],
            recv_sem=line_recv.at[chunk, src],
            device_id={"ep": lax.rem(ep, 4) + 4 * to},
            device_id_type=MESH,
        )

    def near_copy(chunk):
        return pltpu.make_async_remote_copy(
            src_ref=leave_near.at[chunk],
            dst_ref=come_near.at[chunk],
            send_sem=near_send.at[chunk],
            recv_sem=near_recv.at[chunk],
            device_id={"ep": near_peer},
            device_id_type=MESH,
        )

    def level_at(d):
        return lax.rem(level + d, line)

    @pl.loop(0, chunks)
    def _(chunk):
        cols = pl.ds(pl.multiple_of(chunk * width, width), width)
        total = dot(hid_in[0], wd[0:ff_part, cols])
        for j in range(1, n_tp):
            total = total + dot(hid_in[j], wd[j * ff_part : (j + 1) * ff_part, cols])
        given = total.astype(jnp.bfloat16).astype(jnp.float32) * column
        whole[...] = given + dot(sh_hid, sd[:, cols])

        @pl.loop(0, half)
        def _(k):
            owner = 4 * (k // 2) + near * lax.rem(k, 2)
            at = pl.ds(pl.multiple_of(k * rows, rows), rows)
            kept = pl.multiple_of((owner + far * far_bit) * rows, rows)
            sent = pl.multiple_of((owner + far * (1 - far_bit)) * rows, rows)
            keep[chunk, at, :] = whole[pl.ds(kept, rows), :]
            leave_far[chunk, at, :] = whole[pl.ds(sent, rows), :].astype(jnp.bfloat16)

        far_copy(chunk).start()

    @pl.loop(0, chunks)
    def _(chunk):
        far_copy(chunk).wait()
        both = keep[chunk] + come_far[chunk].astype(jnp.float32)
        keep[chunk] = both
        leave_line[chunk] = both.astype(jnp.bfloat16)

        @pl.loop(1, line)
        def _(d):
            line_copy(chunk, level, level_at(d)).start()

    @pl.loop(0, chunks)
    def _(chunk):
        @pl.loop(1, line)
        def _(d):
            line_copy(chunk, level_at(d), level_at(d)).wait()

        def add(d, total):
            src = pl.multiple_of(level_at(d) * pair, pair)
            return total + come_line[chunk, pl.ds(src, pair), :].astype(jnp.float32)

        keep[chunk, here, :] = lax.fori_loop(1, line, add, keep[chunk, here, :])
        other = pl.multiple_of(level * pair + (1 - near_bit) * rows, rows)
        leave_near[chunk] = keep[chunk, pl.ds(other, rows), :]
        near_copy(chunk).start()

    for chunk in range(chunks):
        near_copy(chunk).wait()
        mine_at = pl.multiple_of(level * pair + near_bit * rows, rows)
        done = keep[chunk, pl.ds(mine_at, rows), :] + come_near[chunk]
        out[:, chunk * width : (chunk + 1) * width] = done.astype(jnp.bfloat16)


def on_device(n_ep, n_tp, *args):
    (tokens, ids, slot, rw, eg, eu, ed, sg, su, sd) = args
    rows, feats = tokens.shape
    experts = slot.shape[0]
    ff = eg.shape[2]
    sff = sg.shape[1]
    assert n_ep % 4 == 0
    everyone = rows * n_ep
    ff_part = ff // n_tp
    chunks = math.gcd(feats // 128, 7)
    width = feats // chunks
    bf, f32 = jnp.bfloat16, jnp.float32
    dma = pltpu.SemaphoreType.DMA
    vmem = pl.BlockSpec(memory_space=pltpu.VMEM)
    hbm = pl.BlockSpec(memory_space=pl.ANY)
    return pl.pallas_call(
        functools.partial(kernel, n_ep, n_tp, chunks),
        out_shape=jax.ShapeDtypeStruct((rows, feats), bf),
        in_specs=[vmem] * 3 + [hbm] * 7,
        out_specs=vmem,
        scratch_shapes=[
            pltpu.VMEM((everyone, feats), bf),
            pltpu.VMEM((n_tp, feats, ff_part), bf),
            pltpu.VMEM((n_tp, feats, ff_part), bf),
            pltpu.VMEM((ff, feats), bf),
            pltpu.VMEM((2 * sff + experts, feats), bf),
            pltpu.VMEM((sff, feats), bf),
            pltpu.VMEM((rows, experts), f32),
            pltpu.VMEM((n_tp, rows, experts), f32),
            pltpu.VMEM((rows, experts), f32),
            pltpu.VMEM((everyone, experts), f32),
            pltpu.VMEM((n_tp, 2, everyone, ff_part), f32),
            pltpu.VMEM((n_tp, 2, everyone, ff_part), f32),
            pltpu.VMEM((everyone, 2 * sff), f32),
            pltpu.VMEM((n_tp, everyone, 2 * sff), f32),
            pltpu.VMEM((everyone, ff_part), bf),
            pltpu.VMEM((n_tp, everyone, ff_part), bf),
            pltpu.VMEM((everyone, width), f32),
            pltpu.VMEM((chunks, everyone // 2, width), f32),
            pltpu.VMEM((chunks, everyone // 2, width), bf),
            pltpu.VMEM((chunks, everyone // 2, width), bf),
            pltpu.VMEM((chunks, everyone // 2, width), bf),
            pltpu.VMEM((chunks, everyone // 2, width), bf),
            pltpu.VMEM((chunks, rows, width), f32),
            pltpu.VMEM((chunks, rows, width), f32),
            dma((5 + 2 * n_tp,)),
            dma((1,)),
            dma((4, n_ep)),
            dma((n_ep,)),
            dma((n_tp,)),
            dma((n_tp,)),
            dma((n_ep,)),
            dma((n_ep,)),
            dma((n_tp,)),
            dma((n_tp,)),
            dma((n_tp,)),
            dma((n_tp,)),
            dma((n_tp,)),
            dma((n_tp,)),
            dma((chunks,)),
            dma((chunks,)),
            dma((chunks, n_ep // 4)),
            dma((chunks, n_ep // 4)),
            dma((chunks,)),
            dma((chunks,)),
        ],
        compiler_params=pltpu.CompilerParams(
            collective_id=0, has_side_effects=True, vmem_limit_bytes=63 * 1024 * 1024
        ),
    )(tokens, ids.T, slot[None, :], rw.T, eg, eu, ed, sg.T, su.T, sd)


def solution(mesh):
    placed = (
        P("ep", "tp"),
        P("ep", None),
        P(),
        P("tp", None),
        P("ep", "tp", None),
        P("ep", "tp", None),
        P("ep", None, "tp"),
        P("tp", "ep"),
        P("tp", "ep"),
        P("ep", "tp"),
    )
    return jax.shard_map(
        functools.partial(on_device, mesh.shape["ep"], mesh.shape["tp"]),
        mesh=mesh,
        in_specs=placed,
        out_specs=P("ep", "tp"),
        check_vma=False,
    )
```
